32 devices in a mesh: row: 16 (over z, y, core), col: 2 (over x).
Axes of the slice: x: 2, y: 2, z: 4, core: 2. Of those that a mesh axis runs over, the one named last changes fastest.
Arguments:
- kernel: float32 [5120, 65536], P('row', 'col'), may hold values from -0.0234375 to 0.0234375
- slip: float32 [512, 65536], P('row', 'col'), may hold values from -6 to 6
- segment: int32 [5120], P(('row', 'col')), may hold values from 0 to 15
- prestress: float32 [5120, 512], P(('row', 'col')), may hold values from -4 to 4
- state: float32 [5120, 512], P(('row', 'col')), may hold values from 0.5 to 2
- normal_stress: float32 [5120], P(('row', 'col')), may hold values from 2 to 8
- a_table: float32 [16], replicated, may hold values from 0.5 to 1
- b_table: float32 [16], replicated, may hold values from 0.5 to 1
Outputs:
- new_rate: float32 [5120, 512], P(('row', 'col'))
- new_state: float32 [5120, 512], P(('row', 'col'))
The draws below stay inside these ranges and needn't reach their ends.
All inputs are finite; a program needn't handle non-finite values.
Results may differ from the reference program's by a relative error of at most 0.00016.
Values sent between devices are 32-bit elements; how exact they have to be, the bound alone decides.
A program may use at most 192 MiB of HBM per device.

```python
import math
import jax
import jax.numpy as jnp
from jax import lax

N = 65536
MEMBERS = 512
SEGS = 16
M = 5120


def place_ends(drawn, key, smallest, high):
    place = [jax.random.randint(jax.random.fold_in(key, axis), (), 0, length) for axis, length in enumerate(drawn.shape)]
    widest = drawn.shape.index(max(drawn.shape))
    beside = place[:widest] + [(place[widest] + 1) % drawn.shape[widest]] + place[widest + 1:]
    return drawn.at[tuple(place)].set(smallest).at[tuple(beside)].set(high)


def block_levels(rng, dims, shards, smallest, top_value):
    def one(axis_at, blocks):
        steps = jax.random.uniform(jax.random.fold_in(jax.random.fold_in(rng, 6), axis_at), (blocks,), jnp.float32, smallest / len(shards), top_value / len(shards))
        return jnp.repeat(jnp.exp(steps), dims[axis_at] // blocks).reshape((-1,) + (1,) * (len(dims) - axis_at - 1))

    gain = one(*shards[0])
    for cut in shards[1:]:
        gain = gain * one(*cut)
    return gain


def gaussian(own_key, extent, scale, limit, cuts=(), held_as=jnp.bfloat16):
    values = jax.random.normal(own_key, extent, jnp.float32) * scale
    if len(cuts) > 0:
        values = block_levels(own_key, extent, cuts, -0.22, 0.18) * values
    return jnp.clip(values, min=-limit, max=limit).astype(held_as)


def setup_inputs(seed: int = 0) -> dict:
    seeds = jax.random.split(jax.random.key(seed), 9)
    return {
        "kernel": gaussian(seeds[0], (M, N), N ** -0.5, 0.0234375, ((0, 16), (1, 2)), jnp.float32),
        "slip": gaussian(seeds[1], (MEMBERS, N), 1.0, 6.0, ((0, 16), (1, 2)), jnp.float32),
        "segment": place_ends(jax.random.randint(seeds[2], (M,), 0, SEGS), jax.random.fold_in(seeds[2], 1), 0, SEGS - 1).astype(jnp.int32),
        "prestress": gaussian(seeds[3], (M, MEMBERS), 0.5, 4.0, ((0, 32),), jnp.float32),
        "state": jnp.clip(jnp.exp(math.log(2.0) - 1.3862944 * jax.random.uniform(seeds[4], (M, MEMBERS), jnp.float32) ** block_levels(seeds[4], (M, MEMBERS), ((0, 32),), -0.2, 0.2)), 0.5, 2.0),
        "normal_stress": jnp.clip(jnp.exp(math.log(8.0) - 1.3862944 * jax.random.uniform(seeds[5], (M,), jnp.float32) ** block_levels(seeds[5], (M,), ((0, 32),), -0.2, 0.2)), 2.0, 8.0),
        "a_table": jnp.clip(jnp.exp(jax.random.uniform(seeds[6], (SEGS,), jnp.float32, math.log(0.5), math.log(1.0))), 0.5, 1.0),
        "b_table": jnp.clip(jnp.exp(jax.random.uniform(seeds[7], (SEGS,), jnp.float32, math.log(0.5), math.log(1.0))), 0.5, 1.0),
    }


def reference(kernel, slip, segment, prestress, state, normal_stress, a_table, b_table):
    traction = lax.dot_general(kernel, slip, (((1,), (1,)), ((), ())), precision=lax.Precision.HIGHEST, preferred_element_type=jnp.float32)
    onehot = (segment[:, None] == jnp.arange(SEGS, dtype=jnp.int32)[None, :]).astype(jnp.float32)
    a_rows = jnp.dot(onehot, a_table, precision=lax.Precision.HIGHEST)
    b_rows = jnp.dot(onehot, b_table, precision=lax.Precision.HIGHEST)
    stress = prestress + traction
    new_rate = jnp.exp(-(b_rows / a_rows)[:, None] * jnp.log(state)) * jnp.sinh(stress / (a_rows * normal_stress)[:, None])
    new_state = state + 0.1 * (1.0 - new_rate * state)
    return new_rate, new_state
```

```python
import functools

import jax
import jax.numpy as jnp
from jax import lax
from jax.experimental import pallas as pl
from jax.experimental.pallas import tpu as pltpu
from jax.sharding import PartitionSpec as P

CHUNKS = 16
MESH = pl.DeviceIdType.MESH


def split(value):
    high = value.astype(jnp.bfloat16)
    return high, (value - high.astype(jnp.float32)).astype(jnp.bfloat16)


def times(left, right):
    return lax.dot_general(
        left, right, (((1,), (1,)), ((), ())), preferred_element_type=jnp.float32
    )


def gather_product(
    rows, kernel_ref, slip_ref, total, held, slip_in, kernel_in,
    ring_send, ring_recv, pair_send, pair_recv, own_send, own_recv, slip_sem, kernel_sem,
):
    members = slip_ref.shape[0]
    width = slip_ref.shape[1] // CHUNKS
    chips = rows // 2
    rounds = chips - 1
    pairs = CHUNKS // 2
    me = lax.axis_index("row")
    core = lax.rem(me, 2)
    other = me + 1 - 2 * core
    chip = me // 2
    odd = chip % 2
    place = (1 - odd) * (chip // 2) + odd * (chips - 1 - chip // 2)

    def row_at(spot, which):
        spot = (spot + chips) % chips
        back = spot // (chips // 2)
        return ((1 - back) * 2 * spot + back * (2 * (chips - 1 - spot) + 1)) * 2 + which

    def block(ref, row, chunk):
        return ref.at[
            pl.ds(pl.multiple_of(row * members, members), members),
            pl.ds(pl.multiple_of(chunk * width, width), width),
        ]

    def own(chunk):
        return slip_ref.at[:, pl.ds(pl.multiple_of(chunk * width, width), width)]

    def chunk_of(pair, way, step):
        return 2 * pair + (step + way) % 2

    def origin(way, hops):
        return place - hops if way == 0 else place + hops

    def ring(pair, way, step):
        chunk = chunk_of(pair, way, step)
        hops = step // 2
        row = row_at(origin(way, hops), core)
        return pltpu.make_async_remote_copy(
            src_ref=own(chunk) if hops == 0 else block(held, row, chunk),
            dst_ref=block(held, row, chunk),
            send_sem=ring_send.at[way, step],
            recv_sem=ring_recv.at[pair % 2, way, step],
            device_id={"row": row_at(place + 1 if way == 0 else place - 1, core)},
            device_id_type=MESH,
        )

    def across(pair, way, step):
        chunk = chunk_of(pair, way, step)
        piece = block(held, row_at(origin(way, step // 2 + 1), core), chunk)
        return pltpu.make_async_remote_copy(
            src_ref=piece,
            dst_ref=piece,
            send_sem=pair_send.at[way, step],
            recv_sem=pair_recv.at[pair % 3, way, step],
            device_id={"row": other},
            device_id_type=MESH,
        )

    def across_own(pair, side):
        chunk = 2 * pair + side
        return pltpu.make_async_remote_copy(
            src_ref=own(chunk),
            dst_ref=block(held, me, chunk),
            send_sem=own_send.at[side],
            recv_sem=own_recv.at[pair % 3, side],
            device_id={"row": other},
            device_id_type=MESH,
        )

    def kernel_load(chunk, side):
        return pltpu.make_async_copy(
            kernel_ref.at[:, pl.ds(pl.multiple_of(chunk * width, width), width)],
            kernel_in.at[side],
            kernel_sem.at[side],
        )

    def slip_start(chunk, side):
        def place_in(row):
            return slip_in.at[side, pl.ds(pl.multiple_of(row * members, members), members)]

        pltpu.make_async_copy(own(chunk), place_in(me), slip_sem.at[side]).start()

        def one(at, carry):
            row = (me + at) % rows
            pltpu.make_async_copy(
                block(held, row, chunk), place_in(row), slip_sem.at[side]
            ).start()
            return carry

        lax.fori_loop(1, rows, one, 0)

    def slip_wait(chunk, side):
        pltpu.make_async_copy(
            held.at[:, pl.ds(pl.multiple_of(chunk * width, width), width)],
            slip_in.at[side],
            slip_sem.at[side],
        ).wait()

    depth = min(width, 512)

    def product(side):
        def one(at, carry):
            columns = pl.ds(pl.multiple_of(at * depth, depth), depth)
            k_high, k_low = split(kernel_in[side, :, columns])
            s_high, s_low = split(slip_in[side, :, columns])
            total[...] += times(k_high, s_high) + (times(k_high, s_low) + times(k_low, s_high))
            return carry

        lax.fori_loop(0, width // depth, one, 0)

    total[...] = jnp.zeros_like(total)

    def arrival(pair, way, step):
        ring(pair, way, step).wait_recv()

    def pass_across(pair, way, step):
        @pl.when(pair > 0)
        def _():
            across(pair, way, step).wait_send()

        across(pair, way, step).start()

    def travel(pair, carry):
        sending = pair < pairs
        draining = pair > 0
        for step in range(rounds):

            @pl.when(sending)
            def _():
                for way in range(2):
                    if step >= 2:
                        arrival(pair, way, step - 2)

                    @pl.when(draining)
                    def _():
                        ring(pair, way, step).wait_send()

                    ring(pair, way, step).start()
                if step < 2:

                    @pl.when(draining)
                    def _():
                        across_own(pair, step).wait_send()

                    across_own(pair, step).start()
                else:
                    for way in range(2):
                        pass_across(pair, way, step - 2)

            @pl.when(draining)
            def _():
                if step < 2:
                    for way in range(2):
                        arrival(pair - 1, way, rounds - 2 + step)
                        pass_across(pair - 1, way, rounds - 2 + step)
                if step == 0:
                    for side in range(2):
                        kernel_load(2 * pair - 2 + side, side).start()
                if step == 2:
                    for side in range(2):
                        across_own(pair - 1, side).wait_recv()
                    for way in range(2):
                        for back in range(rounds):
                            across(pair - 1, way, back).wait_recv()
                    for side in range(2):
                        slip_start(2 * pair - 2 + side, side)
                if step in (3, 5):
                    side = (step - 3) // 2
                    kernel_load(2 * pair - 2 + side, side).wait()
                    slip_wait(2 * pair - 2 + side, side)
                    product(side)

        return carry

    lax.fori_loop(0, pairs + 1, travel, 0)
    last = pairs - 1
    for way in range(2):
        for step in range(rounds):
            ring(last, way, step).wait_send()
            across(last, way, step).wait_send()
    for side in range(2):
        across_own(last, side).wait_send()


def traction_partial(rows, kernel, slip):
    targets, columns = kernel.shape
    members = slip.shape[0] * rows
    width = columns // CHUNKS
    rounds = rows // 2 - 1
    dma = pltpu.SemaphoreType.DMA
    flops = 6 * targets * members * columns
    return pl.pallas_call(
        functools.partial(gather_product, rows),
        out_shape=(
            jax.ShapeDtypeStruct((targets, members), jnp.float32),
            jax.ShapeDtypeStruct((members, columns), jnp.float32),
        ),
        in_specs=[pl.BlockSpec(memory_space=pl.ANY)] * 2,
        out_specs=(pl.BlockSpec(memory_space=pltpu.VMEM), pl.BlockSpec(memory_space=pl.ANY)),
        scratch_shapes=[
            pltpu.VMEM((2, members, width), jnp.float32),
            pltpu.VMEM((2, targets, width), jnp.float32),
            dma((2, rounds)),
            dma((2, 2, rounds)),
            dma((2, rounds)),
            dma((3, 2, rounds)),
            dma((2,)),
            dma((3, 2)),
            dma((2,)),
            dma((2,)),
        ],
        compiler_params=pltpu.CompilerParams(
            has_side_effects=True, vmem_limit_bytes=48 * 1024 * 1024
        ),
        cost_estimate=pl.CostEstimate(
            flops=flops, bytes_accessed=4 * members * columns * 4, transcendentals=0
        ),
    )(kernel, slip)[0]


BESIDE, PARTNER, ACROSS = 1, 2, 6
SLOTS = 32
LAG = 2
KERNEL_LAG = 4
LANES = 128
MIDDLE = {
    0: (0, (ACROSS, BESIDE, PARTNER)),
    2: (1, (ACROSS, BESIDE)),
    6: (1, (BESIDE, PARTNER)),
    1: (1, (PARTNER,)),
    3: (2, (ACROSS,)),
    4: (2, (PARTNER,)),
    7: (2, ()),
    5: (3, ()),
}
CORNER = {
    0: (0, (PARTNER, BESIDE)),
    2: (1, (BESIDE,)),
    1: (1, ()),
    4: (2, (BESIDE,)),
    3: (2, ()),
    6: (3, (BESIDE,)),
    5: (3, ()),
    7: (4, ()),
}
SHIPPED = 0


def grid_product(
    rows, kernel_ref, slip_ref, total, held, slip_in, kernel_in, shipped, extra, returned,
    links_send, links_recv, core_send, core_recv, back_send, back_recv, slip_sem, kernel_sem,
):
    members, columns = slip_ref.shape
    width = columns // SLOTS
    layers = rows // 4
    me = lax.axis_index("row")
    core = lax.rem(me, 2)
    other = me + 1 - 2 * core
    chip = me // 2
    side = chip % 2
    layer = chip // 2
    flipped = layer + 1 - 2 * (layer % 2)
    distance = (layer, flipped, (layer + layers // 2) % layers, layers - 1 - layer)
    outer = layer * (layers - 1 - layer) == 0
    inner = jnp.logical_not(outer)
    away = jnp.where(outer, 1, 0)

    def row_of(code):
        beside = side + (1 - 2 * side) * (code % 2)
        return (distance[code // 2] * 2 + beside) * 2 + core

    def ships(parity):
        return width // 8 * (1 + parity)

    def keeps(parity):
        return width - ships(parity)

    pair_ships = ships(0) + ships(1)
    pair_keeps = keeps(0) + keeps(1)

    def block(ref, row, chunk, span):
        return ref.at[
            pl.ds(pl.multiple_of(row * members, members), members),
            pl.ds(pl.multiple_of(chunk * width, width), span),
        ]

    def source(code, chunk, span):
        if code == 0:
            return slip_ref.at[:, pl.ds(pl.multiple_of(chunk * width, width), span)]
        return block(held, row_of(code), chunk, span)

    def sized(count, span):
        return held.at[pl.ds(0, count), pl.ds(0, span)]

    def send(code, link, chunk, span, lane):
        pltpu.make_async_remote_copy(
            src_ref=source(code, chunk, span),
            dst_ref=block(held, row_of(code), chunk, span),
            send_sem=links_send.at[lane],
            recv_sem=links_recv.at[code ^ link, chunk],
            device_id={"row": row_of(link)},
            device_id_type=MESH,
        ).start()

    def arrive(code, chunk, span):
        piece = block(held, row_of(code), chunk, span)
        pltpu.make_async_copy(piece, piece, links_recv.at[code, chunk]).wait()

    def pass_core(code, chunk, span):
        pltpu.make_async_remote_copy(
            src_ref=source(code, chunk, span),
            dst_ref=block(held, row_of(code), chunk, span),
            send_sem=core_send,
            recv_sem=core_recv.at[chunk],
            device_id={"row": other},
            device_id_type=MESH,
        ).start()

    def ship_place(chunk, parity):
        start = chunk // 2 * pair_ships + parity * ships(0)
        return shipped.at[:, pl.ds(pl.multiple_of(start, LANES), ships(parity))]

    def ship(chunk, parity):
        start = chunk * width + keeps(parity)
        return pltpu.make_async_remote_copy(
            src_ref=kernel_ref.at[:, pl.ds(pl.multiple_of(start, LANES), ships(parity))],
            dst_ref=ship_place(chunk, parity),
            send_sem=links_send.at[4],
            recv_sem=links_recv.at[SHIPPED, chunk],
            device_id={"row": row_of(PARTNER)},
            device_id_type=MESH,
        )

    def ship_arrive(chunk, parity):
        piece = ship_place(chunk, parity)
        pltpu.make_async_copy(piece, piece, links_recv.at[SHIPPED, chunk]).wait()

    def move(table, chunk_at, parity, full):
        for code, (hops, links) in table.items():
            chunk = chunk_at - LAG * hops

            @pl.when((chunk >= 0) & (chunk < SLOTS))
            def _():
                mine = width if full else keeps(parity)
                if code:
                    arrive(code, chunk, mine)
                for link in links:
                    if full and link == PARTNER:
                        if code != 1:
                            send(code, link, chunk, keeps(parity), 2)
                        elif parity == 1:
                            send(code, link, chunk, keeps(parity), 3)
                    elif full:
                        send(code, link, chunk, width, 0 if link == ACROSS else 1)
                    elif link == PARTNER:
                        send(code, link, chunk, width, 0)
                    elif code != 2:
                        send(code, link, chunk, keeps(parity), 2)
                    elif parity == 0:
                        send(code, link, chunk, keeps(parity), 3)
                pass_core(code, chunk, mine)

    def load_start(chunk, slot):
        def place_in(row):
            return slip_in.at[slot, pl.ds(pl.multiple_of(row * members, members), members)]

        pltpu.make_async_copy(
            source(0, chunk, width), place_in(me), slip_sem.at[slot]
        ).start()

        def one(at, carry):
            row = (me + at) % rows
            pltpu.make_async_copy(
                block(held, row, chunk, width), place_in(row), slip_sem.at[slot]
            ).start()
            return carry

        lax.fori_loop(1, rows, one, 0)

    def slip_wait(slot):
        pltpu.make_async_copy(
            held.at[:, pl.ds(0, width)], slip_in.at[slot], slip_sem.at[slot]
        ).wait()

    def kernel_load(chunk, slot):
        return pltpu.make_async_copy(
            kernel_ref.at[:, pl.ds(pl.multiple_of(chunk * width, width), width)],
            kernel_in.at[slot],
            kernel_sem.at[slot],
        )

    def three(left, right):
        l_high, l_low = left
        r_high, r_low = right
        return times(l_high, r_high) + (times(l_high, r_low) + times(l_low, r_high))

    def product(chunk, slot, parity):
        depth = ships(1)
        whole = keeps(parity) // depth * depth

        def one(at, carry):
            span = pl.ds(pl.multiple_of(at * depth, depth), depth)
            total[...] += three(split(kernel_in[slot, :, span]), split(slip_in[slot, :, span]))
            return carry

        lax.fori_loop(0, whole // depth, one, 0)
        if keeps(parity) > whole:
            span = pl.ds(whole, keeps(parity) - whole)
            total[...] += three(split(kernel_in[slot, :, span]), split(slip_in[slot, :, span]))

        @pl.when(inner)
        def _():
            ship_arrive(chunk, parity)
            span = pl.ds(keeps(parity), ships(parity))
            slips = split(slip_in[slot, :, span])
            total[...] += three(split(kernel_in[slot, :, span]), slips)
            start = chunk // 2 * pair_ships + parity * ships(0)
            there = pl.ds(pl.multiple_of(start, LANES), ships(parity))
            extra[...] += three(split(shipped[:, there]), slips)

    total[...] = jnp.zeros_like(total)
    extra[...] = jnp.zeros_like(extra)
    last_hop = 3 + away

    def step(at, parity):
        @pl.when(inner)
        def _():
            move(MIDDLE, at, parity, True)

        @pl.when(outer)
        def _():
            move(CORNER, at, parity, False)
            ready = at - KERNEL_LAG

            @pl.when((ready >= 0) & (ready < SLOTS))
            def _():
                ship(ready, parity).start()

        done = at - LAG * last_hop
        following = done - 1
        current = done - 2

        @pl.when((following >= 0) & (following < SLOTS))
        def _():
            slot = 1 - parity
            kernel_load(following, slot).start()

            @pl.when(inner)
            def _():
                piece = sized(members * rows // 2, width)
                pltpu.make_async_copy(piece, piece, core_recv.at[following]).wait()

            @pl.when(outer)
            def _():
                piece = sized(members * rows // 2, keeps(1 - parity))
                pltpu.make_async_copy(piece, piece, core_recv.at[following]).wait()

            load_start(following, slot)

        @pl.when((current >= 0) & (current < SLOTS))
        def _():
            kernel_load(current, parity).wait()
            slip_wait(parity)
            product(current, parity, parity)

    def travel(pair, carry):
        for parity in range(2):
            step(2 * pair + parity, parity)
        return carry

    lax.fori_loop(0, (SLOTS + 4 * LAG + 2) // 2, travel, 0)

    def drained(piece, semaphore):
        pltpu.make_async_copy(piece, piece, semaphore).wait()

    back = pltpu.make_async_remote_copy(
        src_ref=extra,
        dst_ref=returned,
        send_sem=back_send,
        recv_sem=back_recv,
        device_id={"row": row_of(PARTNER)},
        device_id_type=MESH,
    )
    kept = SLOTS // 2 * pair_keeps

    @pl.when(inner)
    def _():
        back.start()
        drained(sized(3 * members, columns), links_send.at[0])
        drained(sized(3 * members, columns), links_send.at[1])
        drained(sized(3 * members, kept), links_send.at[2])
        drained(sized(members, SLOTS // 2 * keeps(1)), links_send.at[3])
        drained(sized(members * rows // 2, columns), core_send)
        back.wait_send()

    @pl.when(outer)
    def _():
        drained(sized(members, columns), links_send.at[0])
        drained(sized(3 * members, kept), links_send.at[2])
        drained(sized(members, SLOTS // 2 * keeps(0)), links_send.at[3])
        drained(shipped, links_send.at[4])
        drained(sized(members * rows // 2, kept), core_send)
        back.wait_recv()
        total[...] += returned[...]


def grid_partial(rows, kernel, slip):
    targets, columns = kernel.shape
    members = slip.shape[0] * rows
    width = columns // SLOTS
    away = SLOTS // 2 * (width // 8 * 3)
    dma = pltpu.SemaphoreType.DMA
    return pl.pallas_call(
        functools.partial(grid_product, rows),
        out_shape=(
            jax.ShapeDtypeStruct((targets, members), jnp.float32),
            jax.ShapeDtypeStruct((members, columns), jnp.float32),
        ),
        in_specs=[pl.BlockSpec(memory_space=pl.ANY)] * 2,
        out_specs=(pl.BlockSpec(memory_space=pltpu.VMEM), pl.BlockSpec(memory_space=pl.ANY)),
        scratch_shapes=[
            pltpu.VMEM((2, members, width), jnp.float32),
            pltpu.VMEM((2, targets, width), jnp.float32),
            pltpu.VMEM((targets, away), jnp.float32),
            pltpu.VMEM((targets, members), jnp.float32),
            pltpu.VMEM((targets, members), jnp.float32),
            dma((5,)),
            dma((8, SLOTS)),
            dma,
            dma((SLOTS,)),
            dma,
            dma,
            dma((2,)),
            dma((2,)),
        ],
        compiler_params=pltpu.CompilerParams(
            has_side_effects=True, vmem_limit_bytes=48 * 1024 * 1024
        ),
        cost_estimate=pl.CostEstimate(
            flops=6 * targets * members * columns,
            bytes_accessed=4 * members * columns * 4,
            transcendentals=0,
        ),
    )(kernel, slip)[0]


def partial_sums(rows, kernel, slip):
    if rows // 4 == 4 and kernel.shape[1] % (SLOTS * 8 * LANES) == 0:
        return grid_partial(rows, kernel, slip)
    return traction_partial(rows, kernel, slip)


def add_over_columns(partial_value, columns):
    if columns != 2:
        return lax.psum_scatter(partial_value, "col", scatter_dimension=0, tiled=True)
    half = partial_value.shape[0] // 2
    me = lax.axis_index("col")
    mine = lax.dynamic_slice_in_dim(partial_value, me * half, half, 0)
    theirs = lax.dynamic_slice_in_dim(partial_value, (1 - me) * half, half, 0)
    return mine + lax.ppermute(theirs, "col", [(0, 1), (1, 0)])


def friction(traction, segment, prestress, state, normal_stress, a_table, b_table):
    onehot = (segment[:, None] == jnp.arange(a_table.shape[0], dtype=jnp.int32)[None, :]).astype(
        jnp.float32
    )
    a_rows = jnp.dot(onehot, a_table, precision=lax.Precision.HIGHEST)
    b_rows = jnp.dot(onehot, b_table, precision=lax.Precision.HIGHEST)
    stress = prestress + traction
    new_rate = jnp.exp(-(b_rows / a_rows)[:, None] * jnp.log(state)) * jnp.sinh(
        stress / (a_rows * normal_stress)[:, None]
    )
    new_state = state + 0.1 * (1.0 - new_rate * state)
    return (new_rate, new_state)


def per_device(rows, columns, kernel, slip, segment, prestress, state, normal_stress, a_table, b_table):
    traction = add_over_columns(partial_sums(rows, kernel, slip), columns)
    return friction(traction, segment, prestress, state, normal_stress, a_table, b_table)


def solution(mesh):
    placed = (
        P("row", "col"),
        P("row", "col"),
        P(("row", "col")),
        P(("row", "col"), None),
        P(("row", "col"), None),
        P(("row", "col")),
        P(),
        P(),
    )
    return jax.shard_map(
        functools.partial(per_device, mesh.shape["row"], mesh.shape["col"]),
        mesh=mesh,
        in_specs=placed,
        out_specs=(P(("row", "col"), None), P(("row", "col"), None)),
        check_vma=False,
    )
```

```python
import functools

import jax
import jax.numpy as jnp
from jax import lax
from jax.experimental import pallas as pl
from jax.experimental.pallas import tpu as pltpu
from jax.sharding import PartitionSpec as P

CHUNKS = 16
MESH = pl.DeviceIdType.MESH


def split(value):
    high = value.astype(jnp.bfloat16)
    return high, (value - high.astype(jnp.float32)).astype(jnp.bfloat16)


def times(left, right):
    return lax.dot_general(
        left, right, (((1,), (1,)), ((), ())), preferred_element_type=jnp.float32
    )


def gather_product(
    rows, kernel_ref, slip_ref, total, held, slip_in, kernel_in,
    ring_send, ring_recv, pair_send, pair_recv, own_send, own_recv, slip_sem, kernel_sem,
):
    members = slip_ref.shape[0]
    width = slip_ref.shape[1] // CHUNKS
    chips = rows // 2
    rounds = chips - 1
    pairs = CHUNKS // 2
    me = lax.axis_index("row")
    core = lax.rem(me, 2)
    other = me + 1 - 2 * core
    chip = me // 2
    odd = chip % 2
    place = (1 - odd) * (chip // 2) + odd * (chips - 1 - chip // 2)

    def row_at(spot, which):
        spot = (spot + chips) % chips
        back = spot // (chips // 2)
        return ((1 - back) * 2 * spot + back * (2 * (chips - 1 - spot) + 1)) * 2 + which

    def block(ref, row, chunk):
        return ref.at[
            pl.ds(pl.multiple_of(row * members, members), members),
            pl.ds(pl.multiple_of(chunk * width, width), width),
        ]

    def own(chunk):
        return slip_ref.at[:, pl.ds(pl.multiple_of(chunk * width, width), width)]

    def chunk_of(pair, way, step):
        return 2 * pair + (step + way) % 2

    def origin(way, hops):
        return place - hops if way == 0 else place + hops

    def ring(pair, way, step):
        chunk = chunk_of(pair, way, step)
        hops = step // 2
        row = row_at(origin(way, hops), core)
        return pltpu.make_async_remote_copy(
            src_ref=own(chunk) if hops == 0 else block(held, row, chunk),
            dst_ref=block(held, row, chunk),
            send_sem=ring_send.at[way, step],
            recv_sem=ring_recv.at[pair % 2, way, step],
            device_id={"row": row_at(place + 1 if way == 0 else place - 1, core)},
            device_id_type=MESH,
        )

    def across(pair, way, step):
        chunk = chunk_of(pair, way, step)
        piece = block(held, row_at(origin(way, step // 2 + 1), core), chunk)
        return pltpu.make_async_remote_copy(
            src_ref=piece,
            dst_ref=piece,
            send_sem=pair_send.at[way, step],
            recv_sem=pair_recv.at[pair % 3, way, step],
            device_id={"row": other},
            device_id_type=MESH,
        )

    def across_own(pair, side):
        chunk = 2 * pair + side
        return pltpu.make_async_remote_copy(
            src_ref=own(chunk),
            dst_ref=block(held, me, chunk),
            send_sem=own_send.at[side],
            recv_sem=own_recv.at[pair % 3, side],
            device_id={"row": other},
            device_id_type=MESH,
        )

    def kernel_load(chunk, side):
        return pltpu.make_async_copy(
            kernel_ref.at[:, pl.ds(pl.multiple_of(chunk * width, width), width)],
            kernel_in.at[side],
            kernel_sem.at[side],
        )

    def slip_start(chunk, side):
        def place_in(row):
            return slip_in.at[side, pl.ds(pl.multiple_of(row * members, members), members)]

        pltpu.make_async_copy(own(chunk), place_in(me), slip_sem.at[side]).start()

        def one(at, carry):
            row = (me + at) % rows
            pltpu.make_async_copy(
                block(held, row, chunk), place_in(row), slip_sem.at[side]
            ).start()
            return carry

        lax.fori_loop(1, rows, one, 0)

    def slip_wait(chunk, side):
        pltpu.make_async_copy(
            held.at[:, pl.ds(pl.multiple_of(chunk * width, width), width)],
            slip_in.at[side],
            slip_sem.at[side],
        ).wait()

    depth = min(width, 512)

    def product(side):
        def one(at, carry):
            columns = pl.ds(pl.multiple_of(at * depth, depth), depth)
            k_high, k_low = split(kernel_in[side, :, columns])
            s_high, s_low = split(slip_in[side, :, columns])
            total[...] += times(k_high, s_high) + (times(k_high, s_low) + times(k_low, s_high))
            return carry

        lax.fori_loop(0, width // depth, one, 0)

    total[...] = jnp.zeros_like(total)

    def arrival(pair, way, step):
        ring(pair, way, step).wait_recv()

    def pass_across(pair, way, step):
        @pl.when(pair > 0)
        def _():
            across(pair, way, step).wait_send()

        across(pair, way, step).start()

    def travel(pair, carry):
        sending = pair < pairs
        draining = pair > 0
        for step in range(rounds):

            @pl.when(sending)
            def _():
                for way in range(2):
                    if step >= 2:
                        arrival(pair, way, step - 2)

                    @pl.when(draining)
                    def _():
                        ring(pair, way, step).wait_send()

                    ring(pair, way, step).start()
                if step < 2:

                    @pl.when(draining)
                    def _():
                        across_own(pair, step).wait_send()

                    across_own(pair, step).start()
                else:
                    for way in range(2):
                        pass_across(pair, way, step - 2)

            @pl.when(draining)
            def _():
                if step < 2:
                    for way in range(2):
                        arrival(pair - 1, way, rounds - 2 + step)
                        pass_across(pair - 1, way, rounds - 2 + step)
                if step == 0:
                    for side in range(2):
                        kernel_load(2 * pair - 2 + side, side).start()
                if step == 2:
                    for side in range(2):
                        across_own(pair - 1, side).wait_recv()
                    for way in range(2):
                        for back in range(rounds):
                            across(pair - 1, way, back).wait_recv()
                    for side in range(2):
                        slip_start(2 * pair - 2 + side, side)
                if step in (3, 5):
                    side = (step - 3) // 2
                    kernel_load(2 * pair - 2 + side, side).wait()
                    slip_wait(2 * pair - 2 + side, side)
                    product(side)

        return carry

    lax.fori_loop(0, pairs + 1, travel, 0)
    last = pairs - 1
    for way in range(2):
        for step in range(rounds):
            ring(last, way, step).wait_send()
            across(last, way, step).wait_send()
    for side in range(2):
        across_own(last, side).wait_send()


def traction_partial(rows, kernel, slip):
    targets, columns = kernel.shape
    members = slip.shape[0] * rows
    width = columns // CHUNKS
    rounds = rows // 2 - 1
    dma = pltpu.SemaphoreType.DMA
    flops = 6 * targets * members * columns
    return pl.pallas_call(
        functools.partial(gather_product, rows),
        out_shape=(
            jax.ShapeDtypeStruct((targets, members), jnp.float32),
            jax.ShapeDtypeStruct((members, columns), jnp.float32),
        ),
        in_specs=[pl.BlockSpec(memory_space=pl.ANY)] * 2,
        out_specs=(pl.BlockSpec(memory_space=pltpu.VMEM), pl.BlockSpec(memory_space=pl.ANY)),
        scratch_shapes=[
            pltpu.VMEM((2, members, width), jnp.float32),
            pltpu.VMEM((2, targets, width), jnp.float32),
            dma((2, rounds)),
            dma((2, 2, rounds)),
            dma((2, rounds)),
            dma((3, 2, rounds)),
            dma((2,)),
            dma((3, 2)),
            dma((2,)),
            dma((2,)),
        ],
        compiler_params=pltpu.CompilerParams(
            has_side_effects=True, vmem_limit_bytes=48 * 1024 * 1024
        ),
        cost_estimate=pl.CostEstimate(
            flops=flops, bytes_accessed=4 * members * columns * 4, transcendentals=0
        ),
    )(kernel, slip)[0]


def add_over_columns(partial_value, columns):
    if columns != 2:
        return lax.psum_scatter(partial_value, "col", scatter_dimension=0, tiled=True)
    half = partial_value.shape[0] // 2
    me = lax.axis_index("col")
    mine = lax.dynamic_slice_in_dim(partial_value, me * half, half, 0)
    theirs = lax.dynamic_slice_in_dim(partial_value, (1 - me) * half, half, 0)
    return mine + lax.ppermute(theirs, "col", [(0, 1), (1, 0)])


BESIDE, PARTNER, ACROSS, FAR = 1, 2, 6, 4
SLOTS = 32
LAG = 1
AHEAD = 8
KERNEL_LAG = 0
LANES = 128
MIDDLE = {
    2: (1, (ACROSS, BESIDE)),
    6: (1, (BESIDE, PARTNER)),
    1: (1, (PARTNER,)),
    3: (2, (ACROSS,)),
    4: (2, (PARTNER,)),
    7: (2, ()),
    5: (3, ()),
    0: (0, (ACROSS, BESIDE, PARTNER)),
}
CORNER = {
    2: (1, (BESIDE,)),
    1: (1, ()),
    4: (2, (BESIDE,)),
    3: (2, ()),
    6: (3, (BESIDE,)),
    5: (3, ()),
    7: (4, ()),
    0: (0, (PARTNER, BESIDE)),
}
SHIPPED = 0


def grid_product(
    rows, kernel_ref, slip_ref, out, held, slip_in, kernel_in, shipped, total, extra, crossed,
    returned, links_send, links_recv, core_send, core_recv, back_send, back_recv, pair_send,
    pair_recv, slip_sem, kernel_sem,
):
    members, columns = slip_ref.shape
    width = columns // SLOTS
    layers = rows // 4
    half = out.shape[0]
    me = lax.axis_index("row")
    column = lax.axis_index("col")
    core = lax.rem(me, 2)
    other = me + 1 - 2 * core
    chip = me // 2
    side = chip % 2
    layer = chip // 2
    end = layer // (layers // 2)
    flipped = layer + 1 - 2 * (layer % 2)
    distance = (layer, flipped, (layer + layers // 2) % layers, layers - 1 - layer)
    outer = layer * (layers - 1 - layer) == 0
    inner = jnp.logical_not(outer)
    halves = (end, 1 - end)
    far_lag = jnp.where(outer, 4 * LAG, 3 * LAG + 3 * LAG % 2)
    lags = (2 * LAG, far_lag)

    def row_of(code):
        beside = side + (1 - 2 * side) * (code % 2)
        return (distance[code // 2] * 2 + beside) * 2 + core

    def ships(parity):
        return width // 8 * (1 + parity)

    def keeps(parity):
        return width - ships(parity)

    pair_ships = ships(0) + ships(1)
    pair_keeps = keeps(0) + keeps(1)

    def block(ref, row, chunk, span):
        return ref.at[
            pl.ds(pl.multiple_of(row * members, members), members),
            pl.ds(pl.multiple_of(chunk * width, width), span),
        ]

    def source(code, chunk, span):
        if code == 0:
            return slip_ref.at[:, pl.ds(pl.multiple_of(chunk * width, width), span)]
        return block(held, row_of(code), chunk, span)

    def sized(count, span):
        return held.at[pl.ds(0, count), pl.ds(0, span)]

    def drained(piece, semaphore):
        pltpu.make_async_copy(piece, piece, semaphore).wait()

    def send(code, link, chunk, span, lane):
        pltpu.make_async_remote_copy(
            src_ref=source(code, chunk, span),
            dst_ref=block(held, row_of(code), chunk, span),
            send_sem=links_send.at[lane],
            recv_sem=links_recv.at[code ^ link, chunk],
            device_id={"row": row_of(link)},
            device_id_type=MESH,
        ).start()

    def arrive(code, chunk, span):
        drained(block(held, row_of(code), chunk, span), links_recv.at[code, chunk])

    def pass_core(code, chunk, span):
        pltpu.make_async_remote_copy(
            src_ref=source(code, chunk, span),
            dst_ref=block(held, row_of(code), chunk, span),
            send_sem=core_send,
            recv_sem=core_recv.at[code // FAR, chunk],
            device_id={"row": other},
            device_id_type=MESH,
        ).start()

    def ship_place(chunk, parity):
        start = chunk // 2 * pair_ships + parity * ships(0)
        return shipped.at[:, pl.ds(pl.multiple_of(start, LANES), ships(parity))]

    def ship(chunk, parity):
        start = chunk * width + keeps(parity)
        return pltpu.make_async_remote_copy(
            src_ref=kernel_ref.at[:, pl.ds(pl.multiple_of(start, LANES), ships(parity))],
            dst_ref=ship_place(chunk, parity),
            send_sem=links_send.at[4],
            recv_sem=links_recv.at[SHIPPED, chunk],
            device_id={"row": row_of(PARTNER)},
            device_id_type=MESH,
        )

    def pass_on(code, links, chunk, parity, full):
        if code:
            arrive(code, chunk, width if full else keeps(parity))
        for link in links:
            if full and link == PARTNER:
                if code != 1:
                    send(code, link, chunk, keeps(parity), 2)
                elif parity == 1:
                    send(code, link, chunk, keeps(parity), 3)
            elif full:
                send(code, link, chunk, width, 0 if link == ACROSS else 1)
            elif link == PARTNER:
                send(code, link, chunk, width, 0)
            elif code != 2:
                send(code, link, chunk, keeps(parity), 2)
            elif parity == 0:
                send(code, link, chunk, keeps(parity), 3)
        pass_core(code, chunk, width if full else keeps(parity))

    def move(table, at, parity, full):
        for code, (hops, links) in table.items():
            late = LAG * hops if code else -AHEAD
            chunk = at - late

            @pl.when((chunk >= 0) & (chunk < SLOTS))
            def _():
                pass_on(code, links, chunk, (parity + late) % 2, full)

    def load_start(part, chunk, slot):
        into = slip_in.at[part, slot]
        if part:
            pltpu.make_async_copy(
                held.at[
                    pl.ds(pl.multiple_of(halves[1] * (rows // 2 * members), members), rows // 2 * members),
                    pl.ds(pl.multiple_of(chunk * width, width), width),
                ],
                into,
                slip_sem.at[part, slot],
            ).start()
            return
        first = end * (rows // 2)
        mine = me - first

        def place_in(spot):
            return into.at[pl.ds(pl.multiple_of(spot * members, members), members)]

        pltpu.make_async_copy(
            source(0, chunk, width), place_in(mine), slip_sem.at[part, slot]
        ).start()

        def one(at, carry):
            spot = (mine + at) % (rows // 2)
            pltpu.make_async_copy(
                block(held, first + spot, chunk, width), place_in(spot), slip_sem.at[part, slot]
            ).start()
            return carry

        lax.fori_loop(1, rows // 2, one, 0)

    def slip_wait(part, slot):
        pltpu.make_async_copy(
            sized(rows // 2 * members, width), slip_in.at[part, slot], slip_sem.at[part, slot]
        ).wait()

    def kernel_load(part, chunk, slot):
        return pltpu.make_async_copy(
            kernel_ref.at[:, pl.ds(pl.multiple_of(chunk * width, width), width)],
            kernel_in.at[part, slot],
            kernel_sem.at[part, slot],
        )

    def three(left, right):
        l_high, l_low = left
        r_high, r_low = right
        return times(l_high, r_high) + (times(l_high, r_low) + times(l_low, r_high))

    def product(part, chunk, slot, parity):
        depth = ships(1)
        whole = keeps(parity) // depth * depth
        where = halves[part]

        def add(span):
            total[where] += three(
                split(kernel_in[part, slot, :, span]), split(slip_in[part, slot, :, span])
            )

        def one(at, carry):
            add(pl.ds(pl.multiple_of(at * depth, depth), depth))
            return carry

        lax.fori_loop(0, whole // depth, one, 0)
        if keeps(parity) > whole:
            add(pl.ds(whole, keeps(parity) - whole))

        @pl.when(inner)
        def _():
            if part == 0:
                drained(ship_place(chunk, parity), links_recv.at[SHIPPED, chunk])
            span = pl.ds(keeps(parity), ships(parity))
            slips = split(slip_in[part, slot, :, span])
            total[where] += three(split(kernel_in[part, slot, :, span]), slips)
            start = chunk // 2 * pair_ships + parity * ships(0)
            there = pl.ds(pl.multiple_of(start, LANES), ships(parity))
            extra[where] += three(split(shipped[:, there]), slips)

    def rows_for(which):
        return pl.ds(pl.multiple_of(which * half, half), half)

    def exchange(part):
        where = halves[part]
        return pltpu.make_async_remote_copy(
            src_ref=total.at[where, rows_for(1 - column)],
            dst_ref=crossed.at[where],
            send_sem=pair_send.at[part],
            recv_sem=pair_recv.at[part],
            device_id={"col": 1 - column},
            device_id_type=MESH,
        )

    def give_back(part, turned):
        where = halves[part]
        target = 1 - column if turned else column
        return pltpu.make_async_remote_copy(
            src_ref=extra.at[where, rows_for(target)],
            dst_ref=returned.at[turned, where],
            send_sem=back_send.at[turned, part],
            recv_sem=back_recv.at[turned, part],
            device_id={"row": row_of(PARTNER), "col": target},
            device_id_type=MESH,
        )

    def reduce_start(part):
        @pl.when(inner)
        def _():
            for turned in range(2):
                give_back(part, turned).start()

        exchange(part).start()

    total[...] = jnp.zeros_like(total)
    extra[...] = jnp.zeros_like(extra)

    def step(at, parity):
        @pl.when(inner)
        def _():
            move(MIDDLE, at, parity, True)

        @pl.when(outer)
        def _():
            move(CORNER, at, parity, False)
            ready = at - KERNEL_LAG

            @pl.when((ready >= 0) & (ready < SLOTS))
            def _():
                ship(ready, parity).start()

        for part in range(2):
            done = at - lags[part]
            following = done - 1
            current = done - 2

            @pl.when((following >= 0) & (following < SLOTS))
            def _():
                slot = 1 - parity

                @pl.when(inner)
                def _():
                    drained(sized(rows // 4 * members, width), core_recv.at[part, following])

                @pl.when(outer)
                def _():
                    drained(sized(rows // 4 * members, keeps(slot)), core_recv.at[part, following])

                load_start(part, following, slot)

            @pl.when((current >= 0) & (current < SLOTS))
            def _():
                kernel_load(part, current, parity).wait()
                slip_wait(part, parity)
                product(part, current, parity, parity)

            @pl.when((done >= 0) & (done < SLOTS))
            def _():
                kernel_load(part, done, parity).start()

            @pl.when(current == SLOTS)
            def _():
                reduce_start(part)

    def begin(pair, carry):
        for parity in range(2):
            chunk = 2 * pair + parity

            @pl.when(inner)
            def _():
                pass_on(0, MIDDLE[0][1], chunk, parity, True)

            @pl.when(outer)
            def _():
                pass_on(0, CORNER[0][1], chunk, parity, False)

        return carry

    def travel(pair, carry):
        for parity in range(2):
            step(2 * pair + parity, parity)
        return carry

    lax.fori_loop(0, AHEAD // 2, begin, 0)
    lax.fori_loop(0, (SLOTS + 4 * LAG + 4) // 2, travel, 0)

    kept = SLOTS // 2 * pair_keeps

    @pl.when(inner)
    def _():
        drained(sized(3 * members, columns), links_send.at[0])
        drained(sized(3 * members, columns), links_send.at[1])
        drained(sized(3 * members, kept), links_send.at[2])
        drained(sized(members, SLOTS // 2 * keeps(1)), links_send.at[3])
        drained(sized(members * rows // 2, columns), core_send)

    @pl.when(outer)
    def _():
        drained(sized(members, columns), links_send.at[0])
        drained(sized(3 * members, kept), links_send.at[2])
        drained(sized(members, SLOTS // 2 * keeps(0)), links_send.at[3])
        drained(shipped, links_send.at[4])
        drained(sized(members * rows // 2, kept), core_send)

    span = out.shape[1] // 2
    for part in range(2):
        exchange(part).wait_recv()
    for where in range(2):
        out[:, pl.ds(where * span, span)] = total[where, rows_for(column)] + crossed[where]

    @pl.when(outer)
    def _():
        for part in range(2):
            for turned in range(2):
                give_back(part, turned).wait_recv()
        for where in range(2):
            out[:, pl.ds(where * span, span)] += returned[0, where] + returned[1, where]

    for part in range(2):
        exchange(part).wait_send()

    @pl.when(inner)
    def _():
        for part in range(2):
            for turned in range(2):
                give_back(part, turned).wait_send()


def grid_traction(rows, kernel, slip):
    targets, columns = kernel.shape
    members = slip.shape[0] * rows
    width = columns // SLOTS
    away = SLOTS // 2 * (width // 8 * 3)
    dma = pltpu.SemaphoreType.DMA
    return pl.pallas_call(
        functools.partial(grid_product, rows),
        out_shape=(
            jax.ShapeDtypeStruct((targets // 2, members), jnp.float32),
            jax.ShapeDtypeStruct((members, columns), jnp.float32),
        ),
        in_specs=[pl.BlockSpec(memory_space=pl.ANY)] * 2,
        out_specs=(pl.BlockSpec(memory_space=pltpu.VMEM), pl.BlockSpec(memory_space=pl.ANY)),
        scratch_shapes=[
            pltpu.VMEM((2, 2, members // 2, width), jnp.float32),
            pltpu.VMEM((2, 2, targets, width), jnp.float32),
            pltpu.VMEM((targets, away), jnp.float32),
            pltpu.VMEM((2, targets, members // 2), jnp.float32),
            pltpu.VMEM((2, targets, members // 2), jnp.float32),
            pltpu.VMEM((2, targets // 2, members // 2), jnp.float32),
            pltpu.VMEM((2, 2, targets // 2, members // 2), jnp.float32),
            dma((5,)),
            dma((8, SLOTS)),
            dma,
            dma((2, SLOTS)),
            dma((2, 2)),
            dma((2, 2)),
            dma((2,)),
            dma((2,)),
            dma((2, 2)),
            dma((2, 2)),
        ],
        compiler_params=pltpu.CompilerParams(
            has_side_effects=True, vmem_limit_bytes=48 * 1024 * 1024
        ),
        cost_estimate=pl.CostEstimate(
            flops=6 * targets * members * columns,
            bytes_accessed=4 * members * columns * 4,
            transcendentals=0,
        ),
    )(kernel, slip)[0]


def traction_rows(rows, columns, kernel, slip):
    if rows // 4 == 4 and columns == 2 and kernel.shape[1] % (SLOTS * 8 * LANES) == 0:
        return grid_traction(rows, kernel, slip)
    return add_over_columns(traction_partial(rows, kernel, slip), columns)


def friction(traction, segment, prestress, state, normal_stress, a_table, b_table):
    onehot = (segment[:, None] == jnp.arange(a_table.shape[0], dtype=jnp.int32)[None, :]).astype(
        jnp.float32
    )
    a_rows = jnp.dot(onehot, a_table, precision=lax.Precision.HIGHEST)
    b_rows = jnp.dot(onehot, b_table, precision=lax.Precision.HIGHEST)
    stress = prestress + traction
    new_rate = jnp.exp(-(b_rows / a_rows)[:, None] * jnp.log(state)) * jnp.sinh(
        stress / (a_rows * normal_stress)[:, None]
    )
    new_state = state + 0.1 * (1.0 - new_rate * state)
    return (new_rate, new_state)


def per_device(rows, columns, kernel, slip, segment, prestress, state, normal_stress, a_table, b_table):
    traction = traction_rows(rows, columns, kernel, slip)
    return friction(traction, segment, prestress, state, normal_stress, a_table, b_table)


def solution(mesh):
    placed = (
        P("row", "col"),
        P("row", "col"),
        P(("row", "col")),
        P(("row", "col"), None),
        P(("row", "col"), None),
        P(("row", "col")),
        P(),
        P(),
    )
    return jax.shard_map(
        functools.partial(per_device, mesh.shape["row"], mesh.shape["col"]),
        mesh=mesh,
        in_specs=placed,
        out_specs=(P(("row", "col"), None), P(("row", "col"), None)),
        check_vma=False,
    )
```

```python
import functools

import jax
import jax.numpy as jnp
from jax import lax
from jax.experimental import pallas as pl
from jax.experimental.pallas import tpu as pltpu
from jax.sharding import PartitionSpec as P

CHUNKS = 16
MESH = pl.DeviceIdType.MESH


def split(value):
    high = value.astype(jnp.bfloat16)
    return high, (value - high.astype(jnp.float32)).astype(jnp.bfloat16)


def times(left, right):
    return lax.dot_general(
        left, right, (((1,), (1,)), ((), ())), preferred_element_type=jnp.float32
    )


def gather_product(
    rows, kernel_ref, slip_ref, total, held, slip_in, kernel_in,
    ring_send, ring_recv, pair_send, pair_recv, own_send, own_recv, slip_sem, kernel_sem,
):
    members = slip_ref.shape[0]
    width = slip_ref.shape[1] // CHUNKS
    chips = rows // 2
    rounds = chips - 1
    pairs = CHUNKS // 2
    me = lax.axis_index("row")
    core = lax.rem(me, 2)
    other = me + 1 - 2 * core
    chip = me // 2
    odd = chip % 2
    place = (1 - odd) * (chip // 2) + odd * (chips - 1 - chip // 2)

    def row_at(spot, which):
        spot = (spot + chips) % chips
        back = spot // (chips // 2)
        return ((1 - back) * 2 * spot + back * (2 * (chips - 1 - spot) + 1)) * 2 + which

    def block(ref, row, chunk):
        return ref.at[
            pl.ds(pl.multiple_of(row * members, members), members),
            pl.ds(pl.multiple_of(chunk * width, width), width),
        ]

    def own(chunk):
        return slip_ref.at[:, pl.ds(pl.multiple_of(chunk * width, width), width)]

    def chunk_of(pair, way, step):
        return 2 * pair + (step + way) % 2

    def origin(way, hops):
        return place - hops if way == 0 else place + hops

    def ring(pair, way, step):
        chunk = chunk_of(pair, way, step)
        hops = step // 2
        row = row_at(origin(way, hops), core)
        return pltpu.make_async_remote_copy(
            src_ref=own(chunk) if hops == 0 else block(held, row, chunk),
            dst_ref=block(held, row, chunk),
            send_sem=ring_send.at[way, step],
            recv_sem=ring_recv.at[pair % 2, way, step],
            device_id={"row": row_at(place + 1 if way == 0 else place - 1, core)},
            device_id_type=MESH,
        )

    def across(pair, way, step):
        chunk = chunk_of(pair, way, step)
        piece = block(held, row_at(origin(way, step // 2 + 1), core), chunk)
        return pltpu.make_async_remote_copy(
            src_ref=piece,
            dst_ref=piece,
            send_sem=pair_send.at[way, step],
            recv_sem=pair_recv.at[pair % 3, way, step],
            device_id={"row": other},
            device_id_type=MESH,
        )

    def across_own(pair, side):
        chunk = 2 * pair + side
        return pltpu.make_async_remote_copy(
            src_ref=own(chunk),
            dst_ref=block(held, me, chunk),
            send_sem=own_send.at[side],
            recv_sem=own_recv.at[pair % 3, side],
            device_id={"row": other},
            device_id_type=MESH,
        )

    def kernel_load(chunk, side):
        return pltpu.make_async_copy(
            kernel_ref.at[:, pl.ds(pl.multiple_of(chunk * width, width), width)],
            kernel_in.at[side],
            kernel_sem.at[side],
        )

    def slip_start(chunk, side):
        def place_in(row):
            return slip_in.at[side, pl.ds(pl.multiple_of(row * members, members), members)]

        pltpu.make_async_copy(own(chunk), place_in(me), slip_sem.at[side]).start()

        def one(at, carry):
            row = (me + at) % rows
            pltpu.make_async_copy(
                block(held, row, chunk), place_in(row), slip_sem.at[side]
            ).start()
            return carry

        lax.fori_loop(1, rows, one, 0)

    def slip_wait(chunk, side):
        pltpu.make_async_copy(
            held.at[:, pl.ds(pl.multiple_of(chunk * width, width), width)],
            slip_in.at[side],
            slip_sem.at[side],
        ).wait()

    depth = min(width, 512)

    def product(side):
        def one(at, carry):
            columns = pl.ds(pl.multiple_of(at * depth, depth), depth)
            k_high, k_low = split(kernel_in[side, :, columns])
            s_high, s_low = split(slip_in[side, :, columns])
            total[...] += times(k_high, s_high) + (times(k_high, s_low) + times(k_low, s_high))
            return carry

        lax.fori_loop(0, width // depth, one, 0)

    total[...] = jnp.zeros_like(total)

    def arrival(pair, way, step):
        ring(pair, way, step).wait_recv()

    def pass_across(pair, way, step):
        @pl.when(pair > 0)
        def _():
            across(pair, way, step).wait_send()

        across(pair, way, step).start()

    def travel(pair, carry):
        sending = pair < pairs
        draining = pair > 0
        for step in range(rounds):

            @pl.when(sending)
            def _():
                for way in range(2):
                    if step >= 2:
                        arrival(pair, way, step - 2)

                    @pl.when(draining)
                    def _():
                        ring(pair, way, step).wait_send()

                    ring(pair, way, step).start()
                if step < 2:

                    @pl.when(draining)
                    def _():
                        across_own(pair, step).wait_send()

                    across_own(pair, step).start()
                else:
                    for way in range(2):
                        pass_across(pair, way, step - 2)

            @pl.when(draining)
            def _():
                if step < 2:
                    for way in range(2):
                        arrival(pair - 1, way, rounds - 2 + step)
                        pass_across(pair - 1, way, rounds - 2 + step)
                if step == 0:
                    for side in range(2):
                        kernel_load(2 * pair - 2 + side, side).start()
                if step == 2:
                    for side in range(2):
                        across_own(pair - 1, side).wait_recv()
                    for way in range(2):
                        for back in range(rounds):
                            across(pair - 1, way, back).wait_recv()
                    for side in range(2):
                        slip_start(2 * pair - 2 + side, side)
                if step in (3, 5):
                    side = (step - 3) // 2
                    kernel_load(2 * pair - 2 + side, side).wait()
                    slip_wait(2 * pair - 2 + side, side)
                    product(side)

        return carry

    lax.fori_loop(0, pairs + 1, travel, 0)
    last = pairs - 1
    for way in range(2):
        for step in range(rounds):
            ring(last, way, step).wait_send()
            across(last, way, step).wait_send()
    for side in range(2):
        across_own(last, side).wait_send()


def traction_partial(rows, kernel, slip):
    targets, columns = kernel.shape
    members = slip.shape[0] * rows
    width = columns // CHUNKS
    rounds = rows // 2 - 1
    dma = pltpu.SemaphoreType.DMA
    flops = 6 * targets * members * columns
    return pl.pallas_call(
        functools.partial(gather_product, rows),
        out_shape=(
            jax.ShapeDtypeStruct((targets, members), jnp.float32),
            jax.ShapeDtypeStruct((members, columns), jnp.float32),
        ),
        in_specs=[pl.BlockSpec(memory_space=pl.ANY)] * 2,
        out_specs=(pl.BlockSpec(memory_space=pltpu.VMEM), pl.BlockSpec(memory_space=pl.ANY)),
        scratch_shapes=[
            pltpu.VMEM((2, members, width), jnp.float32),
            pltpu.VMEM((2, targets, width), jnp.float32),
            dma((2, rounds)),
            dma((2, 2, rounds)),
            dma((2, rounds)),
            dma((3, 2, rounds)),
            dma((2,)),
            dma((3, 2)),
            dma((2,)),
            dma((2,)),
        ],
        compiler_params=pltpu.CompilerParams(
            has_side_effects=True, vmem_limit_bytes=48 * 1024 * 1024
        ),
        cost_estimate=pl.CostEstimate(
            flops=flops, bytes_accessed=4 * members * columns * 4, transcendentals=0
        ),
    )(kernel, slip)[0]


def add_over_columns(partial_value, columns):
    if columns != 2:
        return lax.psum_scatter(partial_value, "col", scatter_dimension=0, tiled=True)
    half = partial_value.shape[0] // 2
    me = lax.axis_index("col")
    mine = lax.dynamic_slice_in_dim(partial_value, me * half, half, 0)
    theirs = lax.dynamic_slice_in_dim(partial_value, (1 - me) * half, half, 0)
    return mine + lax.ppermute(theirs, "col", [(0, 1), (1, 0)])


BESIDE, PARTNER, ACROSS = 1, 2, 6
SLOTS = 32
LAG = 2
EXTRA = 2
AHEAD = 8
OWN_LAG = -AHEAD
KERNEL_LAG = 0
LANES = 128
SHIPS = (1, 2)
DIRECT = (False, True)
PHASES = len(SHIPS)
MIDDLE = {2: LAG, 6: LAG, 1: LAG, 3: 2 * LAG, 4: 2 * LAG, 7: 2 * LAG + EXTRA, 5: 3 * LAG + EXTRA}
CORNER = {2: LAG, 1: LAG, 4: 2 * LAG, 3: 2 * LAG, 6: 3 * LAG, 5: 3 * LAG, 7: 4 * LAG}
MIDDLE_SENDS = (
    (2, ACROSS, LAG),
    (2, BESIDE, LAG),
    (6, PARTNER, LAG),
    (4, PARTNER, 2 * LAG),
    (6, BESIDE, LAG + EXTRA),
    (3, ACROSS, 2 * LAG + EXTRA),
    (1, PARTNER, LAG),
    (0, ACROSS, -AHEAD),
    (0, BESIDE, -AHEAD),
    (0, PARTNER, -AHEAD),
)
CORNER_SENDS = (
    (6, BESIDE, 3 * LAG),
    (4, BESIDE, 2 * LAG),
    (2, BESIDE, LAG),
    (0, PARTNER, -AHEAD),
    (0, BESIDE, OWN_LAG),
)
MIDDLE_FAR, CORNER_FAR = (4, 5, 6, 7), (4, 5, 6, 7)
MIDDLE_LAGS = tuple(
    max(late for code, late in MIDDLE.items() if (code in MIDDLE_FAR) == far) for far in (False, True)
)
CORNER_LAGS = tuple(
    max(late for code, late in CORNER.items() if (code in CORNER_FAR) == far) for far in (False, True)
)
LAGS = tuple(max(pair) for pair in zip(MIDDLE_LAGS, CORNER_LAGS))
SHIPPED = 0


def grid_product(
    rows, kernel_ref, slip_ref, out, held, slip_in, kernel_in, shipped, total, extra, crossed,
    returned, links_send, links_recv, core_send, core_recv, back_send, back_recv, pair_send,
    pair_recv, slip_sem, kernel_sem,
):
    members, columns = slip_ref.shape
    width = columns // SLOTS
    layers = rows // 4
    half = out.shape[0]
    me = lax.axis_index("row")
    column = lax.axis_index("col")
    core = lax.rem(me, 2)
    other = me + 1 - 2 * core
    chip = me // 2
    side = chip % 2
    layer = chip // 2
    end = layer // (layers // 2)
    flipped = layer + 1 - 2 * (layer % 2)
    distance = (layer, flipped, (layer + layers // 2) % layers, layers - 1 - layer)
    outer = layer * (layers - 1 - layer) == 0
    inner = jnp.logical_not(outer)
    firsts = (end * (rows // 2), (1 - end) * (rows // 2))
    counts = (rows // 2, rows // 2)

    def row_of(code):
        beside = side + (1 - 2 * side) * (code % 2)
        return (distance[code // 2] * 2 + beside) * 2 + core

    def ships(phase):
        return width // 8 * SHIPS[phase]

    def keeps(phase):
        return width - ships(phase)

    group_ships = sum(map(ships, range(PHASES)))
    group_keeps = sum(map(keeps, range(PHASES)))
    groups = SLOTS // PHASES
    direct = groups * sum(keeps(phase) for phase in range(PHASES) if DIRECT[phase])
    kept = groups * group_keeps

    def block(ref, row, chunk, span):
        return ref.at[
            pl.ds(pl.multiple_of(row * members, members), members),
            pl.ds(pl.multiple_of(chunk * width, width), span),
        ]

    def source(code, chunk, span):
        if code == 0:
            return slip_ref.at[:, pl.ds(pl.multiple_of(chunk * width, width), span)]
        return block(held, row_of(code), chunk, span)

    def sized(count, span):
        return held.at[pl.ds(0, count), pl.ds(0, span)]

    def drained(piece, semaphore):
        pltpu.make_async_copy(piece, piece, semaphore).wait()

    def send(code, link, chunk, phase, full):
        span, lane = keeps(phase), 2
        if full and link != PARTNER:
            span, lane = width, 0 if link == ACROSS else 1
        elif full and code == 1:
            if not DIRECT[phase]:
                return
            lane = 3
        elif not full and link == PARTNER:
            span, lane = width, 0
        elif not full and code == 2:
            if DIRECT[phase]:
                return
            lane = 3
        pltpu.make_async_remote_copy(
            src_ref=source(code, chunk, span),
            dst_ref=block(held, row_of(code), chunk, span),
            send_sem=links_send.at[lane],
            recv_sem=links_recv.at[code ^ link, chunk],
            device_id={"row": row_of(link)},
            device_id_type=MESH,
        ).start()

    def pass_core(code, chunk, span, part):
        pltpu.make_async_remote_copy(
            src_ref=source(code, chunk, span),
            dst_ref=block(held, row_of(code), chunk, span),
            send_sem=core_send,
            recv_sem=core_recv.at[part, chunk],
            device_id={"row": other},
            device_id_type=MESH,
        ).start()

    def ship_place(chunk, phase):
        start = chunk // PHASES * group_ships + sum(map(ships, range(phase)))
        return pl.ds(pl.multiple_of(start, LANES), ships(phase))

    def ship(chunk, phase):
        start = chunk * width + keeps(phase)
        pltpu.make_async_remote_copy(
            src_ref=kernel_ref.at[:, pl.ds(pl.multiple_of(start, LANES), ships(phase))],
            dst_ref=shipped.at[:, ship_place(chunk, phase)],
            send_sem=links_send.at[4],
            recv_sem=links_recv.at[SHIPPED, chunk],
            device_id={"row": row_of(PARTNER)},
            device_id_type=MESH,
        ).start()

    def at_chunk(at, phase, late, act):
        chunk = at - late

        @pl.when((chunk >= 0) & (chunk < SLOTS))
        def _():
            act(chunk, (phase - late) % PHASES)

    def move(arrivals, sends, far, at, phase, full):
        def span(phase):
            return width if full else keeps(phase)

        def sending(late, code=None):
            chosen = [s for s in sends if s[2] == late and (code is None or s[0] == code)]

            def act(chunk, phase):
                for code, link, _ in chosen:
                    send(code, link, chunk, phase, full)

            if chosen:
                at_chunk(at, phase, late, act)

        for code, late in arrivals.items():

            def act(chunk, phase):
                piece = block(held, row_of(code), chunk, span(phase))
                drained(piece, links_recv.at[code, chunk])
                for forwarded, link, when in sends:
                    if forwarded == code and when == late:
                        send(code, link, chunk, phase, full)
                pass_core(code, chunk, span(phase), int(code in far))

            at_chunk(at, phase, late, act)
        for code, link, when in sends:
            if code and when != arrivals[code]:
                at_chunk(
                    at, phase, when, lambda chunk, phase: send(code, link, chunk, phase, full)
                )
        for code, link, when in sends:
            if code == 0:
                at_chunk(at, phase, when, lambda chunk, phase: send(0, link, chunk, phase, full))
        at_chunk(at, phase, 0, lambda chunk, phase: pass_core(0, chunk, span(phase), 0))

    def load_start(part, chunk, slot):
        into = slip_in[part].at[slot]
        if part:
            pltpu.make_async_copy(
                held.at[
                    pl.ds(pl.multiple_of(firsts[1] * members, members), counts[1] * members),
                    pl.ds(pl.multiple_of(chunk * width, width), width),
                ],
                into,
                slip_sem.at[part, slot],
            ).start()
            return
        mine = me - firsts[0]

        def place_in(spot):
            return into.at[pl.ds(pl.multiple_of(spot * members, members), members)]

        pltpu.make_async_copy(
            source(0, chunk, width), place_in(mine), slip_sem.at[part, slot]
        ).start()

        def one(at, carry):
            spot = (mine + at) % counts[0]
            pltpu.make_async_copy(
                block(held, firsts[0] + spot, chunk, width), place_in(spot), slip_sem.at[part, slot]
            ).start()
            return carry

        lax.fori_loop(1, counts[0], one, 0)

    def slip_wait(part, slot):
        pltpu.make_async_copy(
            sized(counts[part] * members, width), slip_in[part].at[slot], slip_sem.at[part, slot]
        ).wait()

    def kernel_load(part, chunk, slot):
        return pltpu.make_async_copy(
            kernel_ref.at[:, pl.ds(pl.multiple_of(chunk * width, width), width)],
            kernel_in.at[part, slot],
            kernel_sem.at[part, slot],
        )

    def three(left, right):
        l_high, l_low = left
        r_high, r_low = right
        return times(l_high, r_high) + (times(l_high, r_low) + times(l_low, r_high))

    def product(part, chunk, slot, phase):
        def both(span):
            return split(kernel_in[part, slot, :, span]), split(slip_in[part][slot, :, span])

        depth = 2 * LANES
        spans = [
            pl.ds(start, min(depth, keeps(phase) - start)) for start in range(0, keeps(phase), depth)
        ]
        for span in spans:
            total[part][...] += three(*both(span))
        if not ships(phase):
            return

        @pl.when(inner)
        def _():
            there = ship_place(chunk, phase)
            if part == 0:
                drained(shipped.at[:, there], links_recv.at[SHIPPED, chunk])
            kernels, slips = both(pl.ds(keeps(phase), ships(phase)))
            total[part][...] += three(kernels, slips)
            extra[part][...] += three(split(shipped[:, there]), slips)

    def rows_for(which):
        return pl.ds(pl.multiple_of(which * half, half), half)

    def exchange(part):
        return pltpu.make_async_remote_copy(
            src_ref=total[part].at[rows_for(1 - column)],
            dst_ref=crossed[part],
            send_sem=pair_send.at[part],
            recv_sem=pair_recv.at[part],
            device_id={"col": 1 - column},
            device_id_type=MESH,
        )

    def give_back(part, turned):
        target = 1 - column if turned else column
        return pltpu.make_async_remote_copy(
            src_ref=extra[part].at[rows_for(target)],
            dst_ref=returned[part].at[turned],
            send_sem=back_send.at[turned, part],
            recv_sem=back_recv.at[turned, part],
            device_id={"row": row_of(PARTNER), "col": target},
            device_id_type=MESH,
        )

    def reduce_start(part):
        @pl.when(inner)
        def _():
            for turned in range(2):
                give_back(part, turned).start()

        exchange(part).start()

    for part in range(2):
        total[part][...] = jnp.zeros_like(total[part])
        extra[part][...] = jnp.zeros_like(extra[part])

    def step(at, phase):
        @pl.when(inner)
        def _():
            move(MIDDLE, MIDDLE_SENDS, MIDDLE_FAR, at, phase, True)

        @pl.when(outer)
        def _():
            move(CORNER, CORNER_SENDS, CORNER_FAR, at, phase, False)

            def act(chunk, phase):
                if ships(phase):
                    ship(chunk, phase)

            at_chunk(at, phase, KERNEL_LAG, act)

        for part in range(2):

            def load(chunk, phase):
                slot = phase % 2

                @pl.when(inner)
                def _():
                    drained(sized(counts[part] // 2 * members, width), core_recv.at[part, chunk])

                @pl.when(outer)
                def _():
                    drained(
                        sized(counts[part] // 2 * members, keeps(phase)), core_recv.at[part, chunk]
                    )

                load_start(part, chunk, slot)

            def multiply(chunk, phase):
                kernel_load(part, chunk, phase % 2).wait()
                slip_wait(part, phase % 2)
                product(part, chunk, phase % 2, phase)

            def fetch(chunk, phase):
                kernel_load(part, chunk, phase % 2).start()

            at_chunk(at, phase, LAGS[part] + 1, load)
            at_chunk(at, phase, LAGS[part] + 2, multiply)
            at_chunk(at, phase, LAGS[part], fetch)

            @pl.when(at - LAGS[part] - 2 == SLOTS)
            def _():
                reduce_start(part)

    def begin(group, carry):
        for phase in range(PHASES):
            chunk = group * PHASES + phase

            @pl.when(inner)
            def _():
                for code, link, late in MIDDLE_SENDS:
                    if late < 0:
                        send(code, link, chunk, phase, True)

            @pl.when(outer)
            def _():
                for code, link, late in CORNER_SENDS:
                    if late < 0:
                        send(code, link, chunk, phase, False)

        return carry

    def travel(group, carry):
        for phase in range(PHASES):
            step(group * PHASES + phase, phase)
        return carry

    lax.fori_loop(0, AHEAD // PHASES, begin, 0)
    lax.fori_loop(0, pl.cdiv(SLOTS + LAGS[1] + 3, PHASES), travel, 0)

    @pl.when(inner)
    def _():
        drained(sized(3 * members, columns), links_send.at[0])
        drained(sized(3 * members, columns), links_send.at[1])
        drained(sized(3 * members, kept), links_send.at[2])
        drained(sized(members, direct), links_send.at[3])
        drained(sized(members * rows // 2, columns), core_send)

    @pl.when(outer)
    def _():
        drained(sized(members, columns), links_send.at[0])
        drained(sized(3 * members, kept), links_send.at[2])
        drained(sized(members, kept - direct), links_send.at[3])
        drained(shipped, links_send.at[4])
        drained(sized(members * rows // 2, kept), core_send)

    spans = [count * members for count in counts]
    for part in range(2):
        exchange(part).wait_recv()

    @pl.when(outer)
    def _():
        for part in range(2):
            for turned in range(2):
                give_back(part, turned).wait_recv()

    for low in range(2):

        @pl.when(end == low)
        def _():
            for part in range(2):
                first = (0, spans[0])[part] if low == 0 else (spans[1], 0)[part]
                there = pl.ds(first, spans[part])
                out[:, there] = total[part][rows_for(column), :] + crossed[part][...]

                @pl.when(outer)
                def _():
                    out[:, there] += returned[part][0] + returned[part][1]

    for part in range(2):
        exchange(part).wait_send()

    @pl.when(inner)
    def _():
        for part in range(2):
            for turned in range(2):
                give_back(part, turned).wait_send()


def grid_traction(rows, kernel, slip):
    targets, columns = kernel.shape
    members = slip.shape[0] * rows
    width = columns // SLOTS
    away = SLOTS // PHASES * (width // 8 * sum(SHIPS))
    parts = (members // 2, members // 2)
    dma = pltpu.SemaphoreType.DMA
    return pl.pallas_call(
        functools.partial(grid_product, rows),
        out_shape=(
            jax.ShapeDtypeStruct((targets // 2, members), jnp.float32),
            jax.ShapeDtypeStruct((members, columns), jnp.float32),
        ),
        in_specs=[pl.BlockSpec(memory_space=pl.ANY)] * 2,
        out_specs=(pl.BlockSpec(memory_space=pltpu.VMEM), pl.BlockSpec(memory_space=pl.ANY)),
        scratch_shapes=[
            [pltpu.VMEM((2, part, width), jnp.float32) for part in parts],
            pltpu.VMEM((2, 2, targets, width), jnp.float32),
            pltpu.VMEM((targets, away), jnp.float32),
            [pltpu.VMEM((targets, part), jnp.float32) for part in parts],
            [pltpu.VMEM((targets, part), jnp.float32) for part in parts],
            [pltpu.VMEM((targets // 2, part), jnp.float32) for part in parts],
            [pltpu.VMEM((2, targets // 2, part), jnp.float32) for part in parts],
            dma((5,)),
            dma((8, SLOTS)),
            dma,
            dma((2, SLOTS)),
            dma((2, 2)),
            dma((2, 2)),
            dma((2,)),
            dma((2,)),
            dma((2, 2)),
            dma((2, 2)),
        ],
        compiler_params=pltpu.CompilerParams(
            has_side_effects=True, vmem_limit_bytes=60 * 1024 * 1024
        ),
        cost_estimate=pl.CostEstimate(
            flops=6 * targets * members * columns,
            bytes_accessed=4 * members * columns * 4,
            transcendentals=0,
        ),
    )(kernel, slip)[0]


def traction_rows(rows, columns, kernel, slip):
    if rows // 4 == 4 and columns == 2 and kernel.shape[1] % (SLOTS * 8 * LANES) == 0:
        return grid_traction(rows, kernel, slip)
    return add_over_columns(traction_partial(rows, kernel, slip), columns)


def friction(traction, segment, prestress, state, normal_stress, a_table, b_table):
    onehot = (segment[:, None] == jnp.arange(a_table.shape[0], dtype=jnp.int32)[None, :]).astype(
        jnp.float32
    )
    a_rows = jnp.dot(onehot, a_table, precision=lax.Precision.HIGHEST)
    b_rows = jnp.dot(onehot, b_table, precision=lax.Precision.HIGHEST)
    stress = prestress + traction
    new_rate = jnp.exp(-(b_rows / a_rows)[:, None] * jnp.log(state)) * jnp.sinh(
        stress / (a_rows * normal_stress)[:, None]
    )
    new_state = state + 0.1 * (1.0 - new_rate * state)
    return (new_rate, new_state)


def per_device(rows, columns, kernel, slip, segment, prestress, state, normal_stress, a_table, b_table):
    traction = traction_rows(rows, columns, kernel, slip)
    return friction(traction, segment, prestress, state, normal_stress, a_table, b_table)


def solution(mesh):
    placed = (
        P("row", "col"),
        P("row", "col"),
        P(("row", "col")),
        P(("row", "col"), None),
        P(("row", "col"), None),
        P(("row", "col")),
        P(),
        P(),
    )
    return jax.shard_map(
        functools.partial(per_device, mesh.shape["row"], mesh.shape["col"]),
        mesh=mesh,
        in_specs=placed,
        out_specs=(P(("row", "col"), None), P(("row", "col"), None)),
        check_vma=False,
    )
```
